32 devices in a mesh: seq: 8 (over z, y), tp: 4 (over x, core).
Axes of the slice: x: 2, y: 2, z: 4, core: 2. Of those that a mesh axis runs over, the one named last changes fastest.
Arguments:
- inputs: bfloat16 [2, 32, 8192], P(None, 'seq', 'tp'), may hold values from -6 to 6
- out_grad: bfloat16 [2, 32, 8192], P(None, 'seq', 'tp'), may hold values from -6 to 6
- gate_weight: bfloat16 [8192, 14848], P('tp', 'seq'), may hold values from -0.0625 to 0.0625
- up_weight: bfloat16 [8192, 14848], P('tp', 'seq'), may hold values from -0.0625 to 0.0625
- down_weight: bfloat16 [14848, 8192], P('seq', 'tp'), may hold values from -0.0625 to 0.0625
Outputs:
- input_grad: bfloat16 [2, 32, 8192], P(None, 'seq', 'tp')
- gate_grad: float32 [8192, 14848], P('tp', 'seq')
- up_grad: float32 [8192, 14848], P('tp', 'seq')
- down_grad: float32 [14848, 8192], P('seq', 'tp')
The draws below stay inside these ranges and needn't reach their ends.
All inputs are finite; a program needn't handle non-finite values.
Results may differ from the reference program's by a relative error of at most 0.0049.
Values may be sent and summed in bfloat16 or wider, within the bound.
A program may use at most 128 MiB of HBM per device.

```python
import jax
import jax.numpy as jnp

D = 8192
FFW = 14848
GROUPS = 2
TC = 32


def steps_of(rng, shape, pieces, least, high):
    factor_of = 1.0
    for axis_at, shards_of in pieces:
        draws = jax.random.uniform(jax.random.fold_in(jax.random.fold_in(rng, 6), axis_at), (shards_of,), jnp.float32, least / len(pieces), high / len(pieces))
        factor_of = factor_of * jnp.repeat(jnp.exp(draws), shape[axis_at] // shards_of).reshape((-1,) + (1,) * (len(shape) - 1 - axis_at))
    return factor_of


def normal_values(own_key, dims, scale, bound, shards=(), kind=jnp.bfloat16):
    array = jax.random.normal(own_key, dims, jnp.float32) * scale
    if len(shards) > 0:
        array = steps_of(own_key, dims, shards, -0.22, 0.18) * array
    return jnp.clip(array, min=-bound, max=bound).astype(kind)


def setup_inputs(seed: int = 0) -> dict:
    key_of = jax.random.split(jax.random.key(seed), 6)
    return {
        "inputs": normal_values(key_of[0], (GROUPS, TC, D), 1.0, 6.0, ((1, 8), (2, 4))),
        "out_grad": normal_values(key_of[1], (GROUPS, TC, D), 1.0, 6.0, ((1, 8), (2, 4))),
        "gate_weight": normal_values(key_of[2], (D, FFW), D ** -0.5, 0.0625, ((0, 4), (1, 8))),
        "up_weight": normal_values(key_of[3], (D, FFW), D ** -0.5, 0.0625, ((0, 4), (1, 8))),
        "down_weight": normal_values(key_of[4], (FFW, D), D ** -0.5, 0.0625, ((0, 8), (1, 4))),
    }


def reference(inputs, out_grad, gate_weight, up_weight, down_weight):
    gate_total = jnp.zeros((D, FFW), jnp.float32)
    up_total = jnp.zeros((D, FFW), jnp.float32)
    down_total = jnp.zeros((FFW, D), jnp.float32)
    results = []
    for index in range(GROUPS):
        block_in = inputs[index]
        block_grad = out_grad[index]
        gate = jnp.dot(block_in, gate_weight, preferred_element_type=jnp.float32)
        up_proj = jnp.dot(block_in, up_weight, preferred_element_type=jnp.float32)
        hidden = (jax.nn.silu(gate) * up_proj).astype(jnp.bfloat16)
        hidden_grad = jnp.dot(block_grad, down_weight.T, preferred_element_type=jnp.float32)
        sig = jax.nn.sigmoid(gate)
        up_unit = (hidden_grad * gate * sig).astype(jnp.bfloat16)
        gate_unit = (hidden_grad * up_proj * sig * (1.0 + gate * (1.0 - sig))).astype(jnp.bfloat16)
        grad_in = jnp.dot(gate_unit, gate_weight.T, preferred_element_type=jnp.float32)
        grad_in = grad_in + jnp.dot(up_unit, up_weight.T, preferred_element_type=jnp.float32)
        results.append(grad_in.astype(jnp.bfloat16))
        gate_total = gate_total + jnp.dot(block_in.T, gate_unit, preferred_element_type=jnp.float32)
        up_total = up_total + jnp.dot(block_in.T, up_unit, preferred_element_type=jnp.float32)
        down_total = down_total + jnp.dot(hidden.T, block_grad, preferred_element_type=jnp.float32)
    return jnp.stack(results), gate_total, up_total, down_total
```

```python
import functools

import jax
import jax.numpy as jnp
from jax import lax
from jax.experimental import pallas as pl
from jax.experimental.pallas import tpu as pltpu
from jax.sharding import PartitionSpec as P

MESH = pl.DeviceIdType.MESH
F32 = jnp.float32
BF16 = jnp.bfloat16
NT = (((1,), (1,)), ((), ()))
CHUNK = 512
LAG = 2


def padded(size):
    return pl.cdiv(size, 128) * 128


def chunks_of(ffw):
    return [(start, min(CHUNK, ffw - start)) for start in range(0, ffw, CHUNK)]


def front_kernel(n_seq, n_tp, x_hbm, dy_hbm, wg_hbm, wu_hbm, wd_hbm,
                 x_out, dy_out, gu_out, uu_out, hid_out, ig_out,
                 raw, own, gath, wg, wu, wd, part, from_core, sendx, from_chip, acts,
                 in_sem, w_sem, z_send, z_recv, y_send, y_recv,
                 c_send, c_recv, r_send, r_recv, f_send, f_recv):
    seq = lax.axis_index("seq")
    tp = lax.axis_index("tp")
    nz, nchip = n_seq // 2, n_tp // 2
    z, y = lax.div(seq, 2), lax.rem(seq, 2)
    chip, core = lax.div(tp, 2), lax.rem(tp, 2)
    blocks, lines = x_hbm.shape[:2]
    ffw = wg_hbm.shape[0]
    half = gu_out.shape[0] // 2
    chunks = chunks_of(ffw)
    weights = (wg, wu, wd)
    at_y = {"seq": z * 2 + (1 - y)}
    at_core = {"tp": chip * 2 + (1 - core)}

    def z_at(k):
        return lax.rem(z + k, nz)

    def chip_at(k):
        return lax.rem(chip + k, nchip)

    reads = [
        pltpu.make_async_copy(src, raw.at[a], in_sem.at[a]) for a, src in enumerate((x_hbm, dy_hbm))
    ]
    for read in reads:
        read.start()
    loads = {}
    order = [(q, c) for c in range(len(chunks)) for q in range(2)]
    order += [(2, c) for c in range(len(chunks))]
    for q, c in order:
        start, width = chunks[c]
        src = (wg_hbm, wu_hbm, wd_hbm)[q]
        loads[q, c] = pltpu.make_async_copy(
            src.at[pl.ds(start, width)], weights[q].at[pl.ds(start, width)], w_sem.at[q, c]
        )
        loads[q, c].start()

    barrier = pltpu.get_barrier_semaphore()
    for k in range(1, nz):
        pl.semaphore_signal(barrier, inc=1, device_id={"seq": z_at(k) * 2 + y}, device_id_type=MESH)
    for k in range(1, nchip):
        pl.semaphore_signal(barrier, inc=1, device_id={"tp": chip_at(k) * 2 + core}, device_id_type=MESH)
    pl.semaphore_signal(barrier, inc=1, device_id=at_y, device_id_type=MESH)
    pl.semaphore_signal(barrier, inc=1, device_id=at_core, device_id_type=MESH)
    for a in range(2):
        reads[a].wait()
        rows = [raw[a, b].astype(F32) for b in range(blocks)]
        own[a] = jnp.concatenate(rows, axis=0).astype(BF16)
    pl.semaphore_wait(barrier, nz - 1 + nchip - 1 + 2)

    def remote(src, dst, send, recv, to):
        return pltpu.make_async_remote_copy(
            src_ref=src, dst_ref=dst, send_sem=send, recv_sem=recv, device_id=to, device_id_type=MESH
        )

    z_copies, y_copies = [], []
    for a in range(2):
        z_copies.append([
            remote(own.at[a], gath.at[a, z, y], z_send.at[a, k], z_recv.at[a, k], {"seq": z_at(k) * 2 + y})
            for k in range(1, nz)
        ])
        over = [remote(own.at[a], gath.at[a, z, y], y_send.at[a, 0], y_recv.at[a, 0], at_y)]
        over += [
            remote(gath.at[a, z_at(nz - k), y], gath.at[a, z_at(nz - k), y],
                   y_send.at[a, k], y_recv.at[a, k], at_y)
            for k in range(1, nz)
        ]
        y_copies.append(over)
    for a in range(2):
        for copy in z_copies[a]:
            copy.start()
        y_copies[a][0].start()
    for a in range(2):
        gath[a, z, y] = own[a]

    def forward(a):
        for k in range(1, nz):
            z_copies[a][k - 1].wait_recv()
            y_copies[a][k].start()

    def arrive(a, out):
        for k in range(nz):
            y_copies[a][k].wait_recv()
        out[...] = gath[a].astype(F32).reshape(out.shape).astype(BF16)

    c_copies, r_copies, f_copies = {}, {}, {}
    for c, (start, width) in enumerate(chunks):
        columns = pl.ds(start, padded(width))
        for q in range(3):
            c_copies[q, c] = remote(
                part.at[q, 1 - core, :, columns], from_core.at[q, :, columns],
                c_send.at[q, c], c_recv.at[q, c], at_core,
            )
            r_copies[q, c] = [
                remote(sendx.at[q, :, columns], from_chip.at[q, k - 1, :, columns],
                       r_send.at[q, c, k], r_recv.at[q, c, k], {"tp": chip_at(k) * 2 + core})
                for k in range(1, nchip)
            ]
        mine = acts.at[core, :, :, columns]
        f_copies[c] = remote(mine, mine, f_send.at[c], f_recv.at[c], at_core)

    def product(q, c):
        start, width = chunks[c]
        loads[q, c].wait()
        left = (x_out, x_out, dy_out)[q]
        val = lax.dot_general(
            left[...], weights[q][pl.ds(start, width), :], NT, preferred_element_type=F32
        )
        part[q, :, :, pl.ds(start, width)] = val.reshape(2, half, width)
        c_copies[q, c].start()

    def reduce_chip(q, c):
        columns = pl.ds(chunks[c][0], padded(chunks[c][1]))
        c_copies[q, c].wait_recv()
        total = part[q, core, :, columns] + from_core[q, :, columns]
        sendx[q, :, columns] = total.astype(BF16)
        for copy in r_copies[q, c]:
            copy.start()

    def activate(c):
        columns = pl.ds(chunks[c][0], padded(chunks[c][1]))
        values = []
        for q in range(3):
            value = part[q, core, :, columns] + from_core[q, :, columns]
            for k in range(1, nchip):
                r_copies[q, c][k - 1].wait_recv()
                value = value + from_chip[q, k - 1, :, columns].astype(F32)
            values.append(value)
        gate, up, grad = values
        sig = jax.nn.sigmoid(gate)
        acts[core, 0, :, columns] = (grad * up * sig * (1.0 + gate * (1.0 - sig))).astype(BF16)
        acts[core, 1, :, columns] = (grad * gate * sig).astype(BF16)
        acts[core, 2, :, columns] = (gate * sig * up).astype(BF16)
        f_copies[c].start()

    def back(c):
        start, width = chunks[c]
        columns = pl.ds(start, width)
        f_copies[c].wait_recv()
        for q, out in enumerate((gu_out, uu_out, hid_out)):
            out[:, columns] = acts[:, q, :, columns].reshape(2 * half, width)
        val = jnp.dot(gu_out[:, columns], wg[columns, :], preferred_element_type=F32)
        val = val + jnp.dot(uu_out[:, columns], wu[columns, :], preferred_element_type=F32)
        if c:
            val = val + ig_out[...]
        ig_out[...] = val

    forward(0)
    forward(1)
    arrive(0, x_out)
    for i, (q, c) in enumerate(order):
        if (q, c) == (2, 0):
            arrive(1, dy_out)
        product(q, c)
        if i >= LAG:
            reduce_chip(*order[i - LAG])
    for q, c in order[-LAG:]:
        reduce_chip(q, c)
    for c in range(len(chunks)):
        activate(c)
        if c:
            back(c - 1)
    back(len(chunks) - 1)

    for a in range(2):
        for copy in z_copies[a] + y_copies[a]:
            copy.wait_send()
    for q, c in order:
        for copy in [c_copies[q, c]] + r_copies[q, c]:
            copy.wait_send()
    for c in range(len(chunks)):
        f_copies[c].wait_send()


def front(n_seq, n_tp, x, dy, wg, wu, wd):
    blocks, lines, width = x.shape
    rows = blocks * lines
    ffw = wg.shape[0]
    tokens = rows * n_seq
    nz, nchip = n_seq // 2, n_tp // 2
    half = tokens // 2
    cols = padded(ffw)
    n_chunks = len(chunks_of(ffw))
    others = max(nchip - 1, 1)
    vmem = pl.BlockSpec(memory_space=pltpu.VMEM)
    hbm = pl.BlockSpec(memory_space=pl.ANY)
    dma = pltpu.SemaphoreType.DMA
    return pl.pallas_call(
        functools.partial(front_kernel, n_seq, n_tp),
        out_shape=[jax.ShapeDtypeStruct((tokens, width), BF16)] * 2
        + [jax.ShapeDtypeStruct((tokens, ffw), BF16)] * 3
        + [jax.ShapeDtypeStruct((tokens, width), F32)],
        in_specs=[hbm] * 5,
        out_specs=[vmem] * 6,
        scratch_shapes=[
            pltpu.VMEM((2, blocks, lines, width), BF16),
            pltpu.VMEM((2, rows, width), BF16),
            pltpu.VMEM((2, nz, 2, rows, width), BF16),
            pltpu.VMEM(wg.shape, BF16),
            pltpu.VMEM(wu.shape, BF16),
            pltpu.VMEM(wd.shape, BF16),
            pltpu.VMEM((3, 2, half, cols), F32),
            pltpu.VMEM((3, half, cols), F32),
            pltpu.VMEM((3, half, cols), BF16),
            pltpu.VMEM((3, others, half, cols), BF16),
            pltpu.VMEM((2, 3, half, cols), BF16),
            dma((2,)),
            dma((3, n_chunks)),
            dma((2, nz)), dma((2, nz)), dma((2, nz)), dma((2, nz)),
            dma((3, n_chunks)), dma((3, n_chunks)),
            dma((3, n_chunks, nchip)), dma((3, n_chunks, nchip)),
            dma((n_chunks,)), dma((n_chunks,)),
        ],
        compiler_params=pltpu.CompilerParams(
            collective_id=0, has_side_effects=True, vmem_limit_bytes=48 * 1024 * 1024
        ),
        cost_estimate=pl.CostEstimate(
            flops=10 * tokens * width * ffw, bytes_accessed=6 * width * ffw, transcendentals=0
        ),
    )(x, dy, wg, wu, wd)


def block_of(rows):
    return max(r for r in range(16, 513, 16) if rows % r == 0)


def weight_kernel(pairs, slots, rows, *refs):
    lefts, rights = refs[:pairs], refs[pairs : 2 * pairs]
    outs = refs[2 * pairs : 3 * pairs]
    stage, sem = refs[3 * pairs :]
    copies = []
    for left, right, out in zip(lefts, rights, outs):
        for start in range(0, out.shape[0], rows):
            slot = len(copies) % slots
            if len(copies) >= slots:
                copies[-slots].wait()
            turned = left[:, pl.ds(start, rows)].astype(F32).T.astype(BF16)
            stage[slot] = jnp.dot(turned, right[...], preferred_element_type=F32)
            copy = pltpu.make_async_copy(stage.at[slot], out.at[pl.ds(start, rows)], sem.at[slot])
            copy.start()
            copies.append(copy)
    for copy in copies[-slots:]:
        copy.wait()


def weight_grads(lefts, rights):
    tokens, width = rights[0].shape
    ffw = lefts[0].shape[1]
    pairs = len(lefts)
    rows = block_of(ffw)
    slots = min(4, pairs * (ffw // rows))
    return pl.pallas_call(
        functools.partial(weight_kernel, pairs, slots, rows),
        out_shape=[jax.ShapeDtypeStruct((ffw, width), F32)] * pairs,
        in_specs=[pl.BlockSpec(memory_space=pltpu.VMEM)] * (2 * pairs),
        out_specs=[pl.BlockSpec(memory_space=pl.ANY)] * pairs,
        scratch_shapes=[
            pltpu.VMEM((slots, rows, width), F32),
            pltpu.SemaphoreType.DMA((slots,)),
        ],
        compiler_params=pltpu.CompilerParams(vmem_limit_bytes=32 * 1024 * 1024),
        cost_estimate=pl.CostEstimate(
            flops=16 * pairs * tokens * ffw * width,
            bytes_accessed=4 * pairs * ffw * width,
            transcendentals=0,
        ),
    )(*lefts, *rights)


def scatter_sum(n_seq, partial, cover):
    nz = n_seq // 2
    seq = lax.axis_index("seq")
    z, y = seq // 2, lax.rem(seq, 2)
    rows = partial.shape[0] // n_seq
    pieces = partial.reshape(nz, 2, rows, partial.shape[1])
    away = lax.dynamic_index_in_dim(pieces, 1 - y, 1, keepdims=False).astype(BF16)
    kept = lax.dynamic_index_in_dim(pieces, y, 1, keepdims=False)
    arrived = lax.ppermute(away, "seq", [(i, i ^ 1) for i in range(n_seq)])
    kept, *cover = lax.optimization_barrier((kept, *cover))
    summed = kept + arrived.astype(F32)
    result = lax.dynamic_index_in_dim(summed, z, 0, keepdims=False)
    for k in range(1, nz):
        send = lax.dynamic_index_in_dim(summed, lax.rem(z + k, nz), 0, keepdims=False).astype(BF16)
        arrived = lax.ppermute(send, "seq", [(i, (i + 2 * k) % n_seq) for i in range(n_seq)])
        result = result + arrived.astype(F32)
    return result, cover


def solution(mesh):
    n_seq, n_tp = mesh.shape["seq"], mesh.shape["tp"]

    def per_device(inputs, out_grad, gate_weight, up_weight, down_weight):
        x, dy, gate_unit, up_unit, hidden, partial = front(
            n_seq, n_tp, inputs, out_grad, gate_weight.T, up_weight.T, down_weight
        )
        cover = weight_grads((gate_unit,), (x,))
        total, (gate_grad,) = scatter_sum(n_seq, partial, cover)
        up_grad, down_grad = weight_grads((up_unit, hidden), (x, dy))
        return total.astype(BF16).reshape(inputs.shape), gate_grad.T, up_grad.T, down_grad

    return jax.shard_map(
        per_device,
        mesh=mesh,
        in_specs=(
            P(None, "seq", "tp"),
            P(None, "seq", "tp"),
            P("tp", "seq"),
            P("tp", "seq"),
            P("seq", "tp"),
        ),
        out_specs=(P(None, "seq", "tp"), P("tp", "seq"), P("tp", "seq"), P("seq", "tp")),
        check_vma=False,
    )
```

```python
import functools

import jax
import jax.numpy as jnp
from jax import lax
from jax.experimental import pallas as pl
from jax.experimental.pallas import tpu as pltpu
from jax.sharding import PartitionSpec as P

MESH = pl.DeviceIdType.MESH
F32 = jnp.float32
BF16 = jnp.bfloat16
NT = (((1,), (1,)), ((), ()))
CHUNK = 512


def padded(size):
    return pl.cdiv(size, 128) * 128


def pieces_of(size, first):
    cuts, start, width = [], 0, first
    while start < size:
        if size - start - width < 128:
            width = size - start
        cuts.append((start, width))
        start, width = start + width, CHUNK
    return cuts


def chunks_of(ffw):
    return pieces_of(ffw, CHUNK)


def jobs_of(n):
    early, rest = range(min(2, n - 1)), range(min(2, n - 1), n - 1)
    jobs = [([(0, c), (1, c)], turn) for turn in range(2) for c in early]
    if n > 1:
        jobs.append(([(2, c) for c in early], 2))
    jobs += [([(0, c), (1, c)], 2) for c in rest]
    last = [(2, c) for c in rest] + [(0, n - 1), (1, n - 1)]
    return jobs + [(last, 2), ([(2, n - 1)], 2)]


def flipped(i, k, n):
    if n & (n - 1):
        return lax.rem(i + k, n)
    for bit in range(k.bit_length()):
        if k >> bit & 1:
            i = i + (1 - 2 * lax.rem(lax.div(i, 1 << bit), 2)) * (1 << bit)
    return i


def source(i, k, n):
    return flipped(i, n - k if n & (n - 1) else k, n)


def front_kernel(n_seq, n_tp, x_hbm, dy_hbm, wg_hbm, wu_hbm, wd_hbm,
                 x_out, dy_out, gu_out, uu_out, hid_out, ig_out,
                 raw, own, gath, wg, wu, wd, part, from_core, sendx, from_chip, acts, grads,
                 in_sem, w_sem, z_send, z_recv, y_send, y_recv,
                 c_send, c_recv, r_send, r_recv, f_send, f_recv):
    seq = lax.axis_index("seq")
    tp = lax.axis_index("tp")
    nz, nchip = n_seq // 2, n_tp // 2
    z, y = lax.div(seq, 2), lax.rem(seq, 2)
    chip, core = lax.div(tp, 2), lax.rem(tp, 2)
    blocks, lines = x_hbm.shape[:2]
    rows = blocks * lines
    ffw = wg_hbm.shape[0]
    half = gu_out.shape[0] // 2
    chunks = chunks_of(ffw)
    weights = (wg, wu, wd)
    at_y = {"seq": z * 2 + (1 - y)}
    at_core = {"tp": chip * 2 + (1 - core)}

    far_first = range(nz - 1, 0, -1)

    def z_at(k):
        return flipped(z, k, nz)

    def z_from(k):
        return source(z, k, nz)

    def chip_at(k):
        return lax.rem(chip + k, nchip)

    barrier = pltpu.get_barrier_semaphore()
    for k in range(1, nz):
        pl.semaphore_signal(barrier, inc=1, device_id={"seq": z_at(k) * 2 + y}, device_id_type=MESH)
    for k in range(1, nchip):
        pl.semaphore_signal(barrier, inc=1, device_id={"tp": chip_at(k) * 2 + core}, device_id_type=MESH)
    pl.semaphore_signal(barrier, inc=1, device_id=at_y, device_id_type=MESH)
    pl.semaphore_signal(barrier, inc=1, device_id=at_core, device_id_type=MESH)
    reads = [
        pltpu.make_async_copy(src, raw.at[a], in_sem.at[a]) for a, src in enumerate((x_hbm, dy_hbm))
    ]
    for read in reads:
        read.start()
    loads = {}
    jobs = jobs_of(len(chunks))
    order = [(q, c, turn) for items, turn in jobs for q, c in items]
    for q, c, turn in order:
        if turn == 1:
            continue
        start, width = chunks[c]
        src = (wg_hbm, wu_hbm, wd_hbm)[q]
        loads[q, c] = pltpu.make_async_copy(
            src.at[pl.ds(start, width)], weights[q].at[pl.ds(start, width)], w_sem.at[q, c]
        )
        loads[q, c].start(priority=1)


    def settle(a):
        reads[a].wait()
        values = [raw[a, b].astype(F32) for b in range(blocks)]
        own[a] = jnp.concatenate(values, axis=0).astype(BF16)

    settle(0)
    pl.semaphore_wait(barrier, nz - 1 + nchip - 1 + 2)

    def remote(src, dst, send, recv, to):
        return pltpu.make_async_remote_copy(
            src_ref=src, dst_ref=dst, send_sem=send, recv_sem=recv, device_id=to, device_id_type=MESH
        )

    z_copies, y_copies = [], []
    for a in range(2):
        z_copies.append({
            k: remote(own.at[a], gath.at[a, z, y], z_send.at[a, k], z_recv.at[a, k], {"seq": z_at(k) * 2 + y})
            for k in far_first
        })
        over = {0: remote(own.at[a], gath.at[a, z, y], y_send.at[a, 0], y_recv.at[a, 0], at_y)}
        for k in far_first:
            theirs = gath.at[a, z_from(k), y]
            over[k] = remote(theirs, theirs, y_send.at[a, k], y_recv.at[a, k], at_y)
        y_copies.append(over)

    def spread(a):
        for k in far_first:
            z_copies[a][k].start()
        y_copies[a][0].start()
        gath[a, z, y] = own[a]

    def forward(a):
        for k in far_first:
            z_copies[a][k].wait_recv()
            y_copies[a][k].start()

    def arrive(a, out):
        for k in range(nz):
            y_copies[a][k].wait_recv()
        out[...] = gath[a].astype(F32).reshape(out.shape).astype(BF16)

    pairs = nz // 2

    def lines_at(turn):
        return (y, 1 - y, slice(None))[turn]

    c_copies, r_copies, f_copies = {}, {}, {}
    for q, c, turn in order:
        columns = pl.ds(chunks[c][0], padded(chunks[c][1]))
        at = lines_at(turn)
        slot = turn % 2
        c_copies[q, c, turn] = remote(
            part.at[q, pl.ds((1 - core) * pairs, pairs), at, :, columns],
            from_core.at[q, :, at, :, columns],
            c_send.at[q, c, slot], c_recv.at[q, c, slot], at_core,
        )
        r_copies[q, c, turn] = [
            remote(sendx.at[q, :, at, :, columns], from_chip.at[q, k - 1, :, at, :, columns],
                   r_send.at[q, c, slot, k], r_recv.at[q, c, slot, k],
                   {"tp": chip_at(k) * 2 + core})
            for k in range(1, nchip)
        ]
    for c, (start, width) in enumerate(chunks):
        mine = acts.at[core, :, :, pl.ds(start, padded(width))]
        f_copies[c] = remote(mine, mine, f_send.at[c], f_recv.at[c], at_core)

    def multiply(items, turn):
        if turn != 1:
            for item in items:
                loads[item].wait()
        for q, c in items:
            columns = pl.ds(*chunks[c])
            at = lines_at(turn)
            if turn < 2:
                left = gath[q // 2, :, at].astype(F32).reshape(nz * rows, -1).astype(BF16)
            else:
                left = (x_out, x_out, dy_out)[q][...]
            val = lax.dot_general(left, weights[q][columns, :], NT, preferred_element_type=F32)
            shape = (nz, rows) if turn < 2 else (nz, 2, rows)
            part[q, :, at, :, columns] = val.reshape(*shape, chunks[c][1])
        for q, c in items:
            c_copies[q, c, turn].start()

    def reduce_chip(q, c, turn):
        columns = pl.ds(chunks[c][0], padded(chunks[c][1]))
        at = lines_at(turn)
        c_copies[q, c, turn].wait_recv()
        total = part[q, pl.ds(core * pairs, pairs), at, :, columns] + from_core[q, :, at, :, columns]
        sendx[q, :, at, :, columns] = total.astype(BF16)
        for copy in r_copies[q, c, turn]:
            copy.start()

    def activate(c):
        columns = pl.ds(chunks[c][0], padded(chunks[c][1]))
        for turn in range(3):
            for q in range(3):
                for copy in r_copies.get((q, c, turn), []):
                    copy.wait_recv()
        values = []
        for q in range(3):
            value = part[q, pl.ds(core * pairs, pairs), :, :, columns] + from_core[q, :, :, :, columns]
            for k in range(1, nchip):
                value = value + from_chip[q, k - 1, :, :, :, columns].astype(F32)
            values.append(value.reshape(half, -1))
        gate, up, grad = values
        sig = jax.nn.sigmoid(gate)
        acts[core, 0, :, columns] = (grad * up * sig * (1.0 + gate * (1.0 - sig))).astype(BF16)
        acts[core, 1, :, columns] = (grad * gate * sig).astype(BF16)
        acts[core, 2, :, columns] = (gate * sig * up).astype(BF16)
        f_copies[c].start()

    def back(c):
        start, width = chunks[c]
        columns = pl.ds(start, width)
        f_copies[c].wait_recv()
        for q, out in enumerate((gu_out, uu_out, hid_out)):
            out[:, columns] = acts[:, q, :, columns].reshape(2 * half, width)
        val = jnp.dot(gu_out[:, columns], wg[columns, :], preferred_element_type=F32)
        val = val + jnp.dot(uu_out[:, columns], wu[columns, :], preferred_element_type=F32)
        if c:
            val = val + grads[...]
        if c < len(chunks) - 1:
            grads[...] = val
            return
        for i in range(n_seq * blocks):
            ig_out[i // blocks, i % blocks] = val[i * lines : (i + 1) * lines]

    spread(0)
    settle(1)
    forward(0)
    spread(1)
    waiting = []
    late = [i for i, (_, turn) in enumerate(jobs) if turn][0]
    for i, (items, turn) in enumerate(jobs):
        if i == late:
            arrive(0, x_out)
            forward(1)
        if (2, 0) in items:
            arrive(1, dy_out)
        multiply(items, turn)
        for item in waiting:
            reduce_chip(*item)
        waiting = [(q, c, turn) for q, c in items]
    for item in waiting:
        reduce_chip(*item)
    for c in range(len(chunks)):
        activate(c)
        if c:
            back(c - 1)
    back(len(chunks) - 1)

    for a in range(2):
        for copy in [*z_copies[a].values(), *y_copies[a].values()]:
            copy.wait_send()
    for item in order:
        for copy in [c_copies[item]] + r_copies[item]:
            copy.wait_send()
    for c in range(len(chunks)):
        f_copies[c].wait_send()


def front(n_seq, n_tp, x, dy, wg, wu, wd):
    blocks, lines, width = x.shape
    rows = blocks * lines
    ffw = wg.shape[0]
    tokens = rows * n_seq
    nz, nchip = n_seq // 2, n_tp // 2
    half = tokens // 2
    cols = padded(ffw)
    n_chunks = len(chunks_of(ffw))
    others = max(nchip - 1, 1)
    vmem = pl.BlockSpec(memory_space=pltpu.VMEM)
    hbm = pl.BlockSpec(memory_space=pl.ANY)
    dma = pltpu.SemaphoreType.DMA
    return pl.pallas_call(
        functools.partial(front_kernel, n_seq, n_tp),
        out_shape=[jax.ShapeDtypeStruct((tokens, width), BF16)] * 2
        + [jax.ShapeDtypeStruct((tokens, ffw), BF16)] * 3
        + [jax.ShapeDtypeStruct((n_seq, blocks, lines, width), F32)],
        in_specs=[hbm] * 5,
        out_specs=[vmem] * 6,
        scratch_shapes=[
            pltpu.VMEM((2, blocks, lines, width), BF16),
            pltpu.VMEM((2, rows, width), BF16),
            pltpu.VMEM((2, nz, 2, rows, width), BF16),
            pltpu.VMEM(wg.shape, BF16),
            pltpu.VMEM(wu.shape, BF16),
            pltpu.VMEM(wd.shape, BF16),
            pltpu.VMEM((3, nz, 2, rows, cols), F32),
            pltpu.VMEM((3, nz // 2, 2, rows, cols), F32),
            pltpu.VMEM((3, nz // 2, 2, rows, cols), BF16),
            pltpu.VMEM((3, others, nz // 2, 2, rows, cols), BF16),
            pltpu.VMEM((2, 3, half, cols), BF16),
            pltpu.VMEM((tokens, width), F32),
            dma((2,)),
            dma((3, n_chunks)),
            dma((2, nz)), dma((2, nz)), dma((2, nz)), dma((2, nz)),
            dma((3, n_chunks, 2)), dma((3, n_chunks, 2)),
            dma((3, n_chunks, 2, nchip)), dma((3, n_chunks, 2, nchip)),
            dma((n_chunks,)), dma((n_chunks,)),
        ],
        compiler_params=pltpu.CompilerParams(
            collective_id=0, has_side_effects=True, vmem_limit_bytes=48 * 1024 * 1024
        ),
        cost_estimate=pl.CostEstimate(
            flops=10 * tokens * width * ffw, bytes_accessed=6 * width * ffw, transcendentals=0
        ),
    )(x, dy, wg, wu, wd)


def weight_kernel(pairs, slots, *refs):
    lefts, rights = refs[:pairs], refs[pairs : 2 * pairs]
    outs = refs[2 * pairs : 3 * pairs]
    stage, sem = refs[3 * pairs :]
    copies = []
    for left, right, out in zip(lefts, rights, outs):
        for start, rows in pieces_of(out.shape[0], CHUNK if copies else 128):
            slot = len(copies) % slots
            if len(copies) >= slots:
                copies[-slots].wait()
            turned = left[:, pl.ds(start, rows)].astype(F32).T.astype(BF16)
            stage[slot, pl.ds(0, rows)] = jnp.dot(turned, right[...], preferred_element_type=F32)
            copy = pltpu.make_async_copy(
                stage.at[slot, pl.ds(0, rows)], out.at[pl.ds(start, rows)], sem.at[slot]
            )
            copy.start()
            copies.append(copy)
    for copy in copies[-slots:]:
        copy.wait()


def weight_grads(lefts, rights):
    tokens, width = rights[0].shape
    ffw = lefts[0].shape[1]
    pairs = len(lefts)
    cuts = pieces_of(ffw, 128) + pieces_of(ffw, CHUNK) * (pairs - 1)
    slots = min(4, len(cuts))
    return pl.pallas_call(
        functools.partial(weight_kernel, pairs, slots),
        out_shape=[jax.ShapeDtypeStruct((ffw, width), F32)] * pairs,
        in_specs=[pl.BlockSpec(memory_space=pltpu.VMEM)] * (2 * pairs),
        out_specs=[pl.BlockSpec(memory_space=pl.ANY)] * pairs,
        scratch_shapes=[
            pltpu.VMEM((slots, max(rows for _, rows in cuts), width), F32),
            pltpu.SemaphoreType.DMA((slots,)),
        ],
        compiler_params=pltpu.CompilerParams(vmem_limit_bytes=32 * 1024 * 1024),
        cost_estimate=pl.CostEstimate(
            flops=16 * pairs * tokens * ffw * width,
            bytes_accessed=4 * pairs * ffw * width,
            transcendentals=0,
        ),
    )(*lefts, *rights)


def scatter_sum(n_seq, partial, cover):
    nz = n_seq // 2
    seq = lax.axis_index("seq")
    z, y = seq // 2, lax.rem(seq, 2)
    pieces = partial.reshape(nz, 2, *partial.shape[1:])
    away = lax.dynamic_index_in_dim(pieces, 1 - y, 1, keepdims=False).astype(BF16)
    kept = lax.dynamic_index_in_dim(pieces, y, 1, keepdims=False)
    arrived = lax.ppermute(away, "seq", [(i, i ^ 1) for i in range(n_seq)])
    kept, *cover = lax.optimization_barrier((kept, *cover))
    summed = kept + arrived.astype(F32)
    result = lax.dynamic_index_in_dim(summed, z, 0, keepdims=False)
    for k in range(1, nz):
        send = lax.dynamic_index_in_dim(summed, flipped(z, k, nz), 0, keepdims=False).astype(BF16)
        pairs = [
            (i, 2 * (i // 2 ^ k) + i % 2 if nz & (nz - 1) == 0 else (i + 2 * k) % n_seq)
            for i in range(n_seq)
        ]
        result = result + lax.ppermute(send, "seq", pairs).astype(F32)
    return result, cover


def solution(mesh):
    n_seq, n_tp = mesh.shape["seq"], mesh.shape["tp"]

    def per_device(inputs, out_grad, gate_weight, up_weight, down_weight):
        inputs, out_grad = (
            pltpu.with_memory_space_constraint(a, pltpu.HBM) for a in (inputs, out_grad)
        )
        x, dy, gate_unit, up_unit, hidden, partial = front(
            n_seq, n_tp, inputs, out_grad, gate_weight.T, up_weight.T, down_weight
        )
        cover = weight_grads((gate_unit,), (x,))
        total, (gate_grad,) = scatter_sum(n_seq, partial, cover)
        up_grad, down_grad = weight_grads((up_unit, hidden), (x, dy))
        return total.astype(BF16), gate_grad.T, up_grad.T, down_grad

    return jax.shard_map(
        per_device,
        mesh=mesh,
        in_specs=(
            P(None, "seq", "tp"),
            P(None, "seq", "tp"),
            P("tp", "seq"),
            P("tp", "seq"),
            P("seq", "tp"),
        ),
        out_specs=(P(None, "seq", "tp"), P("tp", "seq"), P("tp", "seq"), P("seq", "tp")),
        check_vma=False,
    )
```

```python
import functools

import jax
import jax.numpy as jnp
from jax import lax
from jax.experimental import pallas as pl
from jax.experimental.pallas import tpu as pltpu
from jax.sharding import PartitionSpec as P

MESH = pl.DeviceIdType.MESH
F32 = jnp.float32
BF16 = jnp.bfloat16
NT = (((1,), (1,)), ((), ()))
CHUNK = 512
LAG = 0.9


def padded(size):
    return pl.cdiv(size, 128) * 128


def pieces_of(size, first):
    cuts, start, width = [], 0, first
    while start < size:
        if size - start - width < 128:
            width = size - start
        cuts.append((start, width))
        start, width = start + width, CHUNK
    return cuts


def chunks_of(ffw):
    return pieces_of(ffw, CHUNK)


def jobs_of(n):
    early, rest = range(min(2, n - 1)), range(min(2, n - 1), n)
    jobs = [([(0, c), (1, c)], turn) for turn in range(2) for c in early]
    jobs += [([(0, c), (1, c)], 2) for c in rest]
    if n > 1:
        jobs.append(([(2, c) for c in early], 2))
    return jobs + [([(2, c)], 2) for c in rest]


def flipped(i, k, n):
    if n & (n - 1):
        return lax.rem(i + k, n)
    for bit in range(k.bit_length()):
        if k >> bit & 1:
            i = i + (1 - 2 * lax.rem(lax.div(i, 1 << bit), 2)) * (1 << bit)
    return i


def source(i, k, n):
    return flipped(i, n - k if n & (n - 1) else k, n)


def front_kernel(n_seq, n_tp, x_hbm, dy_hbm, wg_hbm, wu_hbm, wd_hbm,
                 x_out, dy_out, gu_out, uu_out, hid_out, ig_out,
                 raw, own, gath, wg, wu, wd, turned, part, from_core, sendx, from_chip, acts, grads,
                 in_sem, w_sem, z_send, z_recv, y_send, y_recv,
                 c_send, c_recv, r_send, r_recv, f_send, f_recv):
    seq = lax.axis_index("seq")
    tp = lax.axis_index("tp")
    nz, nchip = n_seq // 2, n_tp // 2
    z, y = lax.div(seq, 2), lax.rem(seq, 2)
    chip, core = lax.div(tp, 2), lax.rem(tp, 2)
    blocks, lines = x_hbm.shape[:2]
    rows = blocks * lines
    ffw = wg_hbm.shape[0]
    half = gu_out.shape[0] // 2
    chunks = chunks_of(ffw)
    weights = (wg, wu, wd)
    at_y = {"seq": z * 2 + (1 - y)}
    at_core = {"tp": chip * 2 + (1 - core)}

    far_first = range(nz - 1, 0, -1)

    def z_at(k):
        return flipped(z, k, nz)

    def z_from(k):
        return source(z, k, nz)

    def chip_at(k):
        return lax.rem(chip + k, nchip)

    barrier = pltpu.get_barrier_semaphore()
    for k in range(1, nz):
        pl.semaphore_signal(barrier, inc=1, device_id={"seq": z_at(k) * 2 + y}, device_id_type=MESH)
    for k in range(1, nchip):
        pl.semaphore_signal(barrier, inc=1, device_id={"tp": chip_at(k) * 2 + core}, device_id_type=MESH)
    pl.semaphore_signal(barrier, inc=1, device_id=at_y, device_id_type=MESH)
    pl.semaphore_signal(barrier, inc=1, device_id=at_core, device_id_type=MESH)
    reads = [
        pltpu.make_async_copy(src, raw.at[a], in_sem.at[a]) for a, src in enumerate((x_hbm, dy_hbm))
    ]
    for read in reads:
        read.start()
    loads = {}
    jobs = jobs_of(len(chunks))
    order = [(q, c, turn) for items, turn in jobs for q, c in items]
    for q, c, turn in order:
        if turn == 1:
            continue
        start, width = chunks[c]
        src = (wg_hbm, wu_hbm, wd_hbm)[q]
        loads[q, c] = pltpu.make_async_copy(
            src.at[pl.ds(start, width)], weights[q].at[pl.ds(start, width)], w_sem.at[q, c]
        )
        loads[q, c].start(priority=1)


    def settle(a):
        reads[a].wait()
        values = [raw[a, b].astype(F32) for b in range(blocks)]
        own[a] = jnp.concatenate(values, axis=0).astype(BF16)

    ready, elapsed = set(), []

    def passed(time):
        elapsed[:] = [age + time for age in elapsed]

    def transpose(q, c):
        loads[q, c].wait()
        columns = pl.ds(*chunks[c])
        turned[q, :, columns] = weights[q][columns, :].T
        ready.add((q, c))
        passed(0.59 * chunks[c][1] / CHUNK)

    settle(0)
    pl.semaphore_wait(barrier, nz - 1 + nchip - 1 + 2)

    def remote(src, dst, send, recv, to):
        return pltpu.make_async_remote_copy(
            src_ref=src, dst_ref=dst, send_sem=send, recv_sem=recv, device_id=to, device_id_type=MESH
        )

    z_copies, y_copies = [], []
    for a in range(2):
        z_copies.append({
            k: remote(own.at[a], gath.at[a, z, y], z_send.at[a, k], z_recv.at[a, k], {"seq": z_at(k) * 2 + y})
            for k in far_first
        })
        over = {0: remote(own.at[a], gath.at[a, z, y], y_send.at[a, 0], y_recv.at[a, 0], at_y)}
        for k in far_first:
            theirs = gath.at[a, z_from(k), y]
            over[k] = remote(theirs, theirs, y_send.at[a, k], y_recv.at[a, k], at_y)
        y_copies.append(over)

    def spread(a):
        for k in far_first:
            z_copies[a][k].start()
        y_copies[a][0].start()
        gath[a, z, y] = own[a]

    def forward(a):
        for k in far_first:
            z_copies[a][k].wait_recv()
            y_copies[a][k].start()

    def arrive(a, out):
        for k in range(nz):
            y_copies[a][k].wait_recv()
        out[...] = gath[a].astype(F32).reshape(out.shape).astype(BF16)

    pairs = nz // 2

    def lines_at(turn):
        return (y, 1 - y, slice(None))[turn]

    c_copies, r_copies, f_copies = {}, {}, {}
    for q, c, turn in order:
        columns = pl.ds(chunks[c][0], padded(chunks[c][1]))
        at = lines_at(turn)
        slot = turn % 2
        c_copies[q, c, turn] = remote(
            part.at[q, pl.ds((1 - core) * pairs, pairs), at, :, columns],
            from_core.at[q, :, at, :, columns],
            c_send.at[q, c, slot], c_recv.at[q, c, slot], at_core,
        )
        r_copies[q, c, turn] = [
            remote(sendx.at[q, :, at, :, columns], from_chip.at[q, k - 1, :, at, :, columns],
                   r_send.at[q, c, slot, k], r_recv.at[q, c, slot, k],
                   {"tp": chip_at(k) * 2 + core})
            for k in range(1, nchip)
        ]
    for c, (start, width) in enumerate(chunks):
        mine = acts.at[core, :, :, pl.ds(start, padded(width))]
        f_copies[c] = remote(mine, mine, f_send.at[c], f_recv.at[c], at_core)

    def multiply(items, turn):
        for item in items:
            if item not in ready and turn != 1:
                loads[item].wait()
        passed(sum(0.41 if item in ready else 0.7 for item in items) + 0.25 * (items[0] not in ready))
        for q, c in items:
            columns = pl.ds(*chunks[c])
            at = lines_at(turn)
            if turn < 2:
                left = gath[q // 2, :, at].astype(F32).reshape(nz * rows, -1).astype(BF16)
            else:
                left = (x_out, x_out, dy_out)[q][...]
            if (q, c) in ready:
                val = jnp.dot(left, turned[q, :, columns], preferred_element_type=F32)
            else:
                val = lax.dot_general(left, weights[q][columns, :], NT, preferred_element_type=F32)
            shape = (nz, rows) if turn < 2 else (nz, 2, rows)
            part[q, :, at, :, columns] = val.reshape(*shape, chunks[c][1])
        for q, c in items:
            c_copies[q, c, turn].start()

    def reduce_chip(q, c, turn):
        columns = pl.ds(chunks[c][0], padded(chunks[c][1]))
        at = lines_at(turn)
        c_copies[q, c, turn].wait_recv()
        total = part[q, pl.ds(core * pairs, pairs), at, :, columns] + from_core[q, :, at, :, columns]
        sendx[q, :, at, :, columns] = total.astype(BF16)
        for copy in r_copies[q, c, turn]:
            copy.start()

    def activate(c):
        columns = pl.ds(chunks[c][0], padded(chunks[c][1]))
        for turn in range(3):
            for q in range(3):
                for copy in r_copies.get((q, c, turn), []):
                    copy.wait_recv()
        values = []
        for q in range(3):
            value = part[q, pl.ds(core * pairs, pairs), :, :, columns] + from_core[q, :, :, :, columns]
            for k in range(1, nchip):
                value = value + from_chip[q, k - 1, :, :, :, columns].astype(F32)
            values.append(value.reshape(half, -1))
        gate, up, grad = values
        sig = jax.nn.sigmoid(gate)
        acts[core, 0, :, columns] = (grad * up * sig * (1.0 + gate * (1.0 - sig))).astype(BF16)
        acts[core, 1, :, columns] = (grad * gate * sig).astype(BF16)
        acts[core, 2, :, columns] = (gate * sig * up).astype(BF16)
        f_copies[c].start()

    def back(first, last):
        start = chunks[first][0]
        columns = pl.ds(start, sum(chunks[last]) - start)
        for c in range(first, last + 1):
            f_copies[c].wait_recv()
        for q, out in enumerate((gu_out, uu_out, hid_out)):
            out[:, columns] = acts[:, q, :, columns].reshape(2 * half, columns.size)
        val = jnp.dot(gu_out[:, columns], wg[columns, :], preferred_element_type=F32)
        val = val + jnp.dot(uu_out[:, columns], wu[columns, :], preferred_element_type=F32)
        if first:
            val = val + grads[...]
        if last < len(chunks) - 1:
            grads[...] = val
            return
        for i in range(n_seq * blocks):
            ig_out[i // blocks, i % blocks] = val[i * lines : (i + 1) * lines]

    spread(0)
    settle(1)
    to_turn = [(q, c) for c in range(len(chunks)) for q in range(2)]
    for item in to_turn[:5]:
        transpose(*item)
    forward(0)
    spread(1)
    waiting = []

    def pump(age):
        while waiting and elapsed[0] >= age:
            elapsed.pop(0)
            for item in waiting.pop(0):
                reduce_chip(*item)

    late = [i for i, (_, turn) in enumerate(jobs) if turn][0]
    for i, (items, turn) in enumerate(jobs):
        if i == late:
            for item in to_turn[5:]:
                transpose(*item)
                pump(LAG)
            arrive(0, x_out)
            forward(1)
        if (2, 0) in items:
            pump(0)
            arrive(1, dy_out)
        multiply(items, turn)
        pump(LAG)
        waiting.append([(q, c, turn) for q, c in items])
        elapsed.append(0)
    pump(0)
    for c in range(len(chunks)):
        activate(c)
    for c in range(0, len(chunks), 2):
        back(c, min(c + 1, len(chunks) - 1))

    for a in range(2):
        for copy in [*z_copies[a].values(), *y_copies[a].values()]:
            copy.wait_send()
    for item in order:
        for copy in [c_copies[item]] + r_copies[item]:
            copy.wait_send()
    for c in range(len(chunks)):
        f_copies[c].wait_send()


def front(n_seq, n_tp, x, dy, wg, wu, wd):
    blocks, lines, width = x.shape
    rows = blocks * lines
    ffw = wg.shape[0]
    tokens = rows * n_seq
    nz, nchip = n_seq // 2, n_tp // 2
    half = tokens // 2
    cols = padded(ffw)
    n_chunks = len(chunks_of(ffw))
    others = max(nchip - 1, 1)
    vmem = pl.BlockSpec(memory_space=pltpu.VMEM)
    hbm = pl.BlockSpec(memory_space=pl.ANY)
    dma = pltpu.SemaphoreType.DMA
    return pl.pallas_call(
        functools.partial(front_kernel, n_seq, n_tp),
        out_shape=[jax.ShapeDtypeStruct((tokens, width), BF16)] * 2
        + [jax.ShapeDtypeStruct((tokens, ffw), BF16)] * 3
        + [jax.ShapeDtypeStruct((n_seq, blocks, lines, width), F32)],
        in_specs=[hbm] * 5,
        out_specs=[vmem] * 6,
        scratch_shapes=[
            pltpu.VMEM((2, blocks, lines, width), BF16),
            pltpu.VMEM((2, rows, width), BF16),
            pltpu.VMEM((2, nz, 2, rows, width), BF16),
            pltpu.VMEM(wg.shape, BF16),
            pltpu.VMEM(wu.shape, BF16),
            pltpu.VMEM(wd.shape, BF16),
            pltpu.VMEM((2, width, cols), BF16),
            pltpu.VMEM((3, nz, 2, rows, cols), F32),
            pltpu.VMEM((3, nz // 2, 2, rows, cols), F32),
            pltpu.VMEM((3, nz // 2, 2, rows, cols), BF16),
            pltpu.VMEM((3, others, nz // 2, 2, rows, cols), BF16),
            pltpu.VMEM((2, 3, half, cols), BF16),
            pltpu.VMEM((tokens, width), F32),
            dma((2,)),
            dma((3, n_chunks)),
            dma((2, nz)), dma((2, nz)), dma((2, nz)), dma((2, nz)),
            dma((3, n_chunks, 2)), dma((3, n_chunks, 2)),
            dma((3, n_chunks, 2, nchip)), dma((3, n_chunks, 2, nchip)),
            dma((n_chunks,)), dma((n_chunks,)),
        ],
        compiler_params=pltpu.CompilerParams(
            collective_id=0, has_side_effects=True, vmem_limit_bytes=48 * 1024 * 1024
        ),
        cost_estimate=pl.CostEstimate(
            flops=10 * tokens * width * ffw, bytes_accessed=6 * width * ffw, transcendentals=0
        ),
    )(x, dy, wg, wu, wd)


def steps_of(size, first):
    cuts, start, width = [], 0, 64 if first else 256
    while start < size:
        if size - start - width < 64:
            width = size - start
        cuts.append((start, width))
        start, width = start + width, min(2 * width, 256)
    return cuts


def weight_kernel(pairs, slots, *refs):
    lefts, rights = refs[:pairs], refs[pairs : 2 * pairs]
    outs = refs[2 * pairs : 3 * pairs]
    stage, sem = refs[3 * pairs :]
    copies = []
    for left, right, out in zip(lefts, rights, outs):
        for start, rows in steps_of(out.shape[0], not copies):
            slot = len(copies) % slots
            if len(copies) >= slots:
                copies[-slots].wait()
            turned = left[:, pl.ds(start, rows)].astype(F32).T.astype(BF16)
            stage[slot, pl.ds(0, rows)] = jnp.dot(turned, right[...], preferred_element_type=F32)
            copy = pltpu.make_async_copy(
                stage.at[slot, pl.ds(0, rows)], out.at[pl.ds(start, rows)], sem.at[slot]
            )
            copy.start()
            copies.append(copy)
    for copy in copies[-slots:]:
        copy.wait()


def weight_grads(lefts, rights):
    tokens, width = rights[0].shape
    ffw = lefts[0].shape[1]
    pairs = len(lefts)
    cuts = steps_of(ffw, True) + steps_of(ffw, False) * (pairs - 1)
    slots = min(8, len(cuts))
    return pl.pallas_call(
        functools.partial(weight_kernel, pairs, slots),
        out_shape=[jax.ShapeDtypeStruct((ffw, width), F32)] * pairs,
        in_specs=[pl.BlockSpec(memory_space=pltpu.VMEM)] * (2 * pairs),
        out_specs=[pl.BlockSpec(memory_space=pl.ANY)] * pairs,
        scratch_shapes=[
            pltpu.VMEM((slots, max(rows for _, rows in cuts), width), F32),
            pltpu.SemaphoreType.DMA((slots,)),
        ],
        compiler_params=pltpu.CompilerParams(vmem_limit_bytes=32 * 1024 * 1024),
        cost_estimate=pl.CostEstimate(
            flops=16 * pairs * tokens * ffw * width,
            bytes_accessed=4 * pairs * ffw * width,
            transcendentals=0,
        ),
    )(*lefts, *rights)


def scatter_sum(n_seq, partial, cover):
    nz = n_seq // 2
    seq = lax.axis_index("seq")
    z, y = seq // 2, lax.rem(seq, 2)
    pieces = partial.reshape(nz, 2, *partial.shape[1:])
    away = lax.dynamic_index_in_dim(pieces, 1 - y, 1, keepdims=False).astype(BF16)
    kept = lax.dynamic_index_in_dim(pieces, y, 1, keepdims=False)
    arrived = lax.ppermute(away, "seq", [(i, i ^ 1) for i in range(n_seq)])
    kept, *cover = lax.optimization_barrier((kept, *cover))
    summed = kept + arrived.astype(F32)
    result = lax.dynamic_index_in_dim(summed, z, 0, keepdims=False)
    for k in range(1, nz):
        send = lax.dynamic_index_in_dim(summed, flipped(z, k, nz), 0, keepdims=False).astype(BF16)
        pairs = [
            (i, 2 * (i // 2 ^ k) + i % 2 if nz & (nz - 1) == 0 else (i + 2 * k) % n_seq)
            for i in range(n_seq)
        ]
        result = result + lax.ppermute(send, "seq", pairs).astype(F32)
    return result, cover


def solution(mesh):
    n_seq, n_tp = mesh.shape["seq"], mesh.shape["tp"]

    def per_device(inputs, out_grad, gate_weight, up_weight, down_weight):
        inputs, out_grad = (
            pltpu.with_memory_space_constraint(a, pltpu.HBM) for a in (inputs, out_grad)
        )
        x, dy, gate_unit, up_unit, hidden, partial = front(
            n_seq, n_tp, inputs, out_grad, gate_weight.T, up_weight.T, down_weight
        )
        cover = weight_grads((gate_unit,), (x,))
        total, (gate_grad,) = scatter_sum(n_seq, partial, cover)
        up_grad, down_grad = weight_grads((up_unit, hidden), (x, dy))
        return total.astype(BF16), gate_grad.T, up_grad.T, down_grad

    return jax.shard_map(
        per_device,
        mesh=mesh,
        in_specs=(
            P(None, "seq", "tp"),
            P(None, "seq", "tp"),
            P("tp", "seq"),
            P("tp", "seq"),
            P("seq", "tp"),
        ),
        out_specs=(P(None, "seq", "tp"), P("tp", "seq"), P("tp", "seq"), P("seq", "tp")),
        check_vma=False,
    )
```
